128 devices in a mesh: gx: 4 (over y), gy: 4 (over z_hi, core), gz: 8 (over z_lo, x).
Axes of the slice: x: 4, y: 4, z: 4 (z_hi: 2, z_lo: 2; z = z_hi * 2 + z_lo), core: 2. Of those that a mesh axis runs over, the one named last changes fastest.
Arguments:
- volume: bfloat16 [32, 32, 32, 32, 128], P('gx', 'gy', 'gz'), may hold values from -6 to 6
- conv_kernel: bfloat16 [3, 3, 3, 32, 64], replicated, may hold values from -0.21875 to 0.21875
- dense_one: bfloat16 [16, 16, 16, 64, 2048], P('gx', None, None, ('gy', 'gz')), may hold values from -0.01171875 to 0.01171875
- dense_two: float32 [2048, 256], replicated, may hold values from -0.125 to 0.125
- dense_three: float32 [256, 4], replicated, may hold values from -0.375 to 0.375
- targets: float32 [4, 128], replicated, may hold values from -3 to 3
Outputs:
- prediction: float32 [4, 128], replicated
- grad_dense_one: bfloat16 [16, 16, 16, 64, 2048], P('gx', None, None, ('gy', 'gz'))
- grad_conv: float32 [3, 3, 3, 32, 64], replicated
- grad_volume: bfloat16 [32, 32, 32, 32, 128], P('gx', 'gy', 'gz')
The draws below stay inside these ranges and needn't reach their ends.
All inputs are finite; a program needn't handle non-finite values.
Results may differ from the reference program's by a relative error of at most 0.008.
Values may be sent and summed in bfloat16 or wider, within the bound.
A program may use at most 128 MiB of HBM per device.

```python
import math
import jax
import jax.numpy as jnp
from jax import lax

BATCH = 128
CIN = 32
COUT = 64
HID1 = 2048
HID2 = 256
OUTS = 4
NX = 32
NY = 32
NZ = 32
MX = 16
MY = 16
MZ = 16


def steps_of(rng, shape, pieces, least, top_value):
    def one(position, shards_of):
        draws = jax.random.uniform(jax.random.fold_in(jax.random.fold_in(rng, 6), position), (shards_of,), jnp.float32, least / len(pieces), top_value / len(pieces))
        return jnp.repeat(jnp.exp(draws), shape[position] // shards_of).reshape((-1,) + (1,) * (len(shape) - position - 1))

    factor_of = one(*pieces[0])
    for cut in pieces[1:]:
        factor_of = factor_of * one(*cut)
    return factor_of


def gaussian(key, dims, scale, bound, pieces=(), held_as=jnp.bfloat16):
    values = jax.random.normal(key, dims, jnp.float32) * scale
    if len(pieces) > 0:
        values = steps_of(key, dims, pieces, -0.22, 0.18) * values
    return jnp.clip(values, min=-bound, max=bound).astype(held_as)


def setup_inputs(seed: int = 0) -> dict:
    seeds = jax.random.split(jax.random.key(seed), 7)
    volume = gaussian(seeds[0], (NX, NY, NZ, CIN, BATCH), 1.0, 6.0, ((0, 4), (1, 4), (2, 8)))
    conv_kernel = gaussian(seeds[1], (3, 3, 3, CIN, COUT), (27 * CIN) ** -0.5, 0.21875)
    dense_one = gaussian(seeds[2], (MX, MY, MZ, COUT, HID1), (MX * MY * MZ * COUT) ** -0.5, 0.01171875, ((0, 4), (3, 32)))
    dense_two = gaussian(seeds[3], (HID1, HID2), HID1 ** -0.5, 0.125, (), jnp.float32)
    dense_three = gaussian(seeds[4], (HID2, OUTS), HID2 ** -0.5, 0.375, (), jnp.float32)
    targets = gaussian(seeds[5], (OUTS, BATCH), 0.5, 3.0, (), jnp.float32)
    return {"volume": volume, "conv_kernel": conv_kernel, "dense_one": dense_one, "dense_two": dense_two, "dense_three": dense_three, "targets": targets}


loss_scale = 1024.0
leak_slope = 0.3

def smooth_leaky(values):
    return leak_slope * values + (1.0 - leak_slope) * jax.nn.softplus(values)

def leaky_derivative(values):
    return leak_slope + (1.0 - leak_slope) * jax.nn.sigmoid(values)

def conv_forward(padded, kernel):
    return lax.conv_general_dilated(padded, kernel, (1, 1, 1), 'VALID', dimension_numbers=('DHWCN', 'DHWIO', 'DHWCN'), preferred_element_type=jnp.float32)

def conv_back_input(padded_grad, kernel):
    flipped = kernel[::-1, ::-1, ::-1]
    return lax.conv_general_dilated(padded_grad, flipped, (1, 1, 1), 'VALID', dimension_numbers=('DHWCN', 'DHWOI', 'DHWCN'), preferred_element_type=jnp.float32)

def conv_back_kernel(padded, gradient):
    return lax.conv_general_dilated(padded, gradient, (1, 1, 1), 'VALID', dimension_numbers=('DHWNC', 'DHWOI', 'DHWNC'), preferred_element_type=jnp.float32)

def pooling(values):
    extent_x, extent_y, extent_z, channels, samples = values.shape
    return values.reshape(extent_x // 2, 2, extent_y // 2, 2, extent_z // 2, 2, channels, samples).mean(axis=(1, 3, 5))

def spread(values):
    extent_x, extent_y, extent_z, channels, samples = values.shape
    widened = jnp.broadcast_to(values[:, None, :, None, :, None], (extent_x, 2, extent_y, 2, extent_z, 2, channels, samples))
    return widened.reshape(2 * extent_x, 2 * extent_y, 2 * extent_z, channels, samples)

def split_samples(values, block_count, block_size):
    return jnp.moveaxis(values.reshape(values.shape[:4] + (block_count, block_size)), 4, 0)

def join_samples(values):
    moved = jnp.moveaxis(values, 0, 4)
    return moved.reshape(moved.shape[:4] + (moved.shape[4] * moved.shape[5],))

def reference(volume, conv_kernel, dense_one, dense_two, dense_three, targets):
    samples = volume.shape[4]
    block_size = math.gcd(samples, 16)
    block_count = samples // block_size
    rim = ((1, 1), (1, 1), (1, 1), (0, 0), (0, 0))
    blocks = split_samples(jnp.pad(volume, rim), block_count, block_size)

    def forward_block(padded):
        return pooling(smooth_leaky(conv_forward(padded, conv_kernel))).astype(jnp.bfloat16)
    pooled = join_samples(lax.map(forward_block, blocks))
    features = pooled.reshape(-1, samples)
    weights_flat = dense_one.reshape(-1, dense_one.shape[4])
    pre_one = lax.dot_general(weights_flat, features, (((0,), (0,)), ((), ())), preferred_element_type=jnp.float32)
    hidden_one = smooth_leaky(pre_one)
    pre_two = jnp.dot(dense_two.T, hidden_one, precision=lax.Precision.HIGHEST)
    hidden_two = smooth_leaky(pre_two)
    prediction = jnp.dot(dense_three.T, hidden_two, precision=lax.Precision.HIGHEST)
    error_grad = loss_scale * (prediction - targets)
    grad_pre_two = jnp.dot(dense_three, error_grad, precision=lax.Precision.HIGHEST) * leaky_derivative(pre_two)
    grad_pre_one = (jnp.dot(dense_two, grad_pre_two, precision=lax.Precision.HIGHEST) * leaky_derivative(pre_one)).astype(jnp.bfloat16)

    def slab_grad(slab):
        flat = slab.reshape(-1, samples)
        product = lax.dot_general(flat, grad_pre_one, (((1,), (1,)), ((), ())), preferred_element_type=jnp.float32)
        return (product / samples).astype(jnp.bfloat16).reshape(dense_one.shape[1:])
    grad_dense_one = lax.map(slab_grad, pooled)
    grad_features = jnp.dot(weights_flat, grad_pre_one, preferred_element_type=jnp.float32).astype(jnp.bfloat16)
    grad_blocks = split_samples(grad_features.reshape(pooled.shape), block_count, block_size)

    def backward_block(pair):
        padded, grad_pooled = pair
        conv_out = conv_forward(padded, conv_kernel)
        grad_out = (spread(grad_pooled.astype(jnp.float32)) / 8.0 * leaky_derivative(conv_out)).astype(jnp.bfloat16)
        grad_padded = jnp.pad(grad_out, rim)
        grad_input = conv_back_input(grad_padded, conv_kernel).astype(jnp.bfloat16)
        return (grad_input, conv_back_kernel(padded, grad_out))
    grad_inputs, grad_kernels = lax.map(backward_block, (blocks, grad_blocks))
    grad_conv = lax.optimization_barrier(jnp.sum(grad_kernels, axis=0)) / samples
    grad_volume = join_samples(grad_inputs)
    return (prediction, grad_dense_one, grad_conv, grad_volume)
```

```python
import functools

import jax
import jax.numpy as jnp
from jax import lax
from jax.experimental import pallas as pl
from jax.experimental.pallas import tpu as pltpu
from jax.sharding import PartitionSpec as P

loss_scale = 1024.0
leak_slope = 0.3
MESH = pl.DeviceIdType.MESH


def position():
    gx, gy, gz = lax.axis_index("gx"), lax.axis_index("gy"), lax.axis_index("gz")
    return gx, gy, gz


def chip_coordinates(gx, gy, gz):
    return {"x": gz % 4, "y": gx, "z": (gy // 2) * 2 + gz // 4, "c": gy % 2}


def device_of(at):
    return (at["y"], (at["z"] // 2) * 2 + at["c"], (at["z"] % 2) * 4 + at["x"])


def greet(devices):
    barrier = pltpu.get_barrier_semaphore()
    for device in devices:
        pl.semaphore_signal(barrier, inc=1, device_id=device, device_id_type=MESH)
    pl.semaphore_wait(barrier, len(devices))


def all_reduce_kernel(x_ref, o_ref, from_core, half_sum, from_1, sum_1, from_2, sum_2, from_3,
                      core_send, core_recv, send, recv):
    at = chip_coordinates(*position())
    core = at["c"]
    half = x_ref.shape[0] // 2
    color = half // 2
    n1 = color // 4
    n2 = n1 // 4
    routes = (("x", "y", "z"), ("y", "z", "x"))

    def peer(dim, step):
        other = dict(at)
        other[dim] = (at[dim] + step) % 4
        return other

    partner = dict(at)
    partner["c"] = 1 - core
    greet([device_of(partner)] + [device_of(peer(d, s)) for d in "xyz" for s in (1, 2, 3)])

    def copy(src, dst, s_sem, r_sem, device):
        return pltpu.make_async_remote_copy(
            src_ref=src, dst_ref=dst, send_sem=s_sem, recv_sem=r_sem,
            device_id=device, device_id_type=MESH)

    first = copy(x_ref.at[pl.ds((1 - core) * half, half)], from_core, core_send.at[0],
                 core_recv.at[0], device_of(partner))
    first.start()
    first.wait()
    half_sum[...] = x_ref[pl.ds(core * half, half)] + from_core[...]

    def exchange(stage, source, target):
        copies = []
        for k in range(2):
            for s in (2, 1, 3):
                other = peer(routes[k][min(stage, 4 - stage)], s)
                c = copy(source(k, other), target(k, s), send.at[k, stage, s - 1],
                         recv.at[k, stage, s - 1], device_of(other))
                c.start()
                copies.append(c)
        for c in copies:
            c.wait()

    def me(k, j):
        return at[routes[k][j]]

    exchange(0, lambda k, o: half_sum.at[pl.ds(k * color + o[routes[k][0]] * n1, n1)],
             lambda k, s: from_1.at[k, s - 1])
    for k in range(2):
        sum_1[k] = (half_sum[pl.ds(k * color + me(k, 0) * n1, n1)] + from_1[k, 0]
                    + from_1[k, 1] + from_1[k, 2])
    exchange(1, lambda k, o: sum_1.at[k, pl.ds(o[routes[k][1]] * n2, n2)],
             lambda k, s: from_2.at[k, s - 1])
    for k in range(2):
        sum_2[k] = (sum_1[k, pl.ds(me(k, 1) * n2, n2)] + from_2[k, 0]
                    + from_2[k, 1] + from_2[k, 2])
        from_3[k, me(k, 2)] = sum_2[k]
    exchange(2, lambda k, o: sum_2.at[k], lambda k, s: from_3.at[k, me(k, 2)])
    base = [core * half + k * color + me(k, 0) * n1 for k in range(2)]
    for k in range(2):
        o_ref[pl.ds(base[k] + me(k, 1) * n2, n2)] = (
            from_3[k, 0] + from_3[k, 1] + from_3[k, 2] + from_3[k, 3])

    def spread_rows(stage, start, size):
        exchange(stage, lambda k, o: o_ref.at[pl.ds(start(k), size)],
                 lambda k, s: o_ref.at[pl.ds(start(k), size)])

    spread_rows(3, lambda k: base[k] + me(k, 1) * n2, n2)
    spread_rows(4, lambda k: base[k], n1)
    mine = o_ref.at[pl.ds(core * half, half)]
    last = copy(mine, mine, core_send.at[1], core_recv.at[1], device_of(partner))
    last.start()
    last.wait()


def all_reduce(x, collective):
    rows = x.shape[0]
    half = rows // 2
    n1, n2 = half // 8, half // 32
    f32 = jnp.float32
    return pl.pallas_call(
        all_reduce_kernel,
        out_shape=jax.ShapeDtypeStruct(x.shape, f32),
        in_specs=[pl.BlockSpec(memory_space=pltpu.VMEM)],
        out_specs=pl.BlockSpec(memory_space=pltpu.VMEM),
        scratch_shapes=[
            pltpu.VMEM((half, 128), f32),
            pltpu.VMEM((half, 128), f32),
            pltpu.VMEM((2, 3, n1, 128), f32),
            pltpu.VMEM((2, n1, 128), f32),
            pltpu.VMEM((2, 3, n2, 128), f32),
            pltpu.VMEM((2, n2, 128), f32),
            pltpu.VMEM((2, 4, n2, 128), f32),
            pltpu.SemaphoreType.DMA((2,)),
            pltpu.SemaphoreType.DMA((2,)),
            pltpu.SemaphoreType.DMA((2, 5, 3)),
            pltpu.SemaphoreType.DMA((2, 5, 3)),
        ],
        compiler_params=pltpu.CompilerParams(collective_id=collective, has_side_effects=True),
        name="all_reduce_%d" % collective,
    )(x)


def exchange_kernel(s_ref, r_ref, own_sem, send, recv):
    gx, gy, gz = position()
    me = gy * 8 + gz

    def device(p):
        return (gx, p // 8, p % 8)

    barrier = pltpu.get_barrier_semaphore()

    def hello(k, carry):
        pl.semaphore_signal(barrier, inc=1, device_id=device((me + k) % 32), device_id_type=MESH)
        return carry

    lax.fori_loop(1, 32, hello, 0)
    own = pltpu.make_async_copy(s_ref.at[me], r_ref.at[me], own_sem)
    own.start()
    pl.semaphore_wait(barrier, 31)

    def copy(k, source, target, to):
        return pltpu.make_async_remote_copy(
            src_ref=s_ref.at[source], dst_ref=r_ref.at[target], send_sem=send.at[k],
            recv_sem=recv.at[k], device_id=device(to), device_id_type=MESH)

    def start(k, carry):
        p = (me + k) % 32
        copy(k, p, me, p).start()
        return carry

    lax.fori_loop(1, 32, start, 0)

    def finish(k, carry):
        p = (me + k) % 32
        q = (me + 32 - k) % 32
        copy(k, p, q, p).wait_send()
        copy(k, p, q, p).wait_recv()
        return carry

    lax.fori_loop(1, 32, finish, 0)
    own.wait()


def exchange(blocks, collective):
    return pl.pallas_call(
        exchange_kernel,
        out_shape=jax.ShapeDtypeStruct(blocks.shape, blocks.dtype),
        in_specs=[pl.BlockSpec(memory_space=pltpu.VMEM)],
        out_specs=pl.BlockSpec(memory_space=pltpu.VMEM),
        scratch_shapes=[
            pltpu.SemaphoreType.DMA,
            pltpu.SemaphoreType.DMA((32,)),
            pltpu.SemaphoreType.DMA((32,)),
        ],
        compiler_params=pltpu.CompilerParams(collective_id=collective, has_side_effects=True),
        name="exchange_%d" % collective,
    )(blocks)


def halo_kernel(v_ref, p_ref, own_sem, send, recv):
    gx, gy, gz = position()
    here = {"x": gx, "y": gy, "z": gz}
    size = {"x": 4, "y": 4, "z": 8}
    low = {d: here[d] > 0 for d in "xyz"}
    high = {d: here[d] < size[d] - 1 for d in "xyz"}

    def neighbour(d, step):
        to = dict(here)
        to[d] = (here[d] + size[d] + step) % size[d]
        return (to["x"], to["y"], to["z"])

    zero = jnp.zeros((), p_ref.dtype)

    @pl.when(jnp.logical_not(low["z"]))
    def _():
        p_ref[:, :, 0] = jnp.full(p_ref.shape[:2] + p_ref.shape[3:], zero)

    @pl.when(jnp.logical_not(high["z"]))
    def _():
        p_ref[:, :, 5] = jnp.full(p_ref.shape[:2] + p_ref.shape[3:], zero)

    @pl.when(jnp.logical_not(low["y"]))
    def _():
        p_ref[:, 0] = jnp.full(p_ref.shape[:1] + p_ref.shape[2:], zero)

    @pl.when(jnp.logical_not(high["y"]))
    def _():
        p_ref[:, 9] = jnp.full(p_ref.shape[:1] + p_ref.shape[2:], zero)

    @pl.when(jnp.logical_not(low["x"]))
    def _():
        p_ref[0] = jnp.full(p_ref.shape[1:], zero)

    @pl.when(jnp.logical_not(high["x"]))
    def _():
        p_ref[9] = jnp.full(p_ref.shape[1:], zero)

    greet([neighbour(d, s) for d in "xyz" for s in (1, -1)])
    inner = pl.ds(1, 8)
    mid = pl.ds(1, 4)
    own = pltpu.make_async_copy(v_ref, p_ref.at[inner, inner, mid], own_sem)
    own.start()

    pending = []

    def transfer(slot, d, up, source, target, extra):
        copy = pltpu.make_async_remote_copy(
            src_ref=source, dst_ref=target, send_sem=send.at[slot], recv_sem=recv.at[slot],
            device_id=neighbour(d, 1 if up else -1), device_id_type=MESH)
        sends = high[d] if up else low[d]
        gets = low[d] if up else high[d]
        if extra is not None:
            sends, gets = jnp.logical_and(sends, extra), jnp.logical_and(gets, extra)
        pl.when(sends)(copy.start)
        pending.append((sends, copy))
        return lambda: pl.when(gets)(copy.wait_recv)

    arrive = {}
    arrive["z", 0] = transfer(0, "z", True, v_ref.at[:, :, 3], p_ref.at[inner, inner, 0], None)
    arrive["z", 1] = transfer(1, "z", False, v_ref.at[:, :, 0], p_ref.at[inner, inner, 5], None)
    arrive["y", 0] = transfer(2, "y", True, v_ref.at[:, 7], p_ref.at[inner, 0, mid], None)
    arrive["y", 1] = transfer(3, "y", False, v_ref.at[:, 0], p_ref.at[inner, 9, mid], None)
    arrive["x", 0] = transfer(4, "x", True, v_ref.at[7], p_ref.at[0, inner, mid], None)
    arrive["x", 1] = transfer(5, "x", False, v_ref.at[0], p_ref.at[9, inner, mid], None)

    later = []
    for side, plane in ((0, 0), (1, 5)):
        arrive["z", side]()
        has = low["z"] if side == 0 else high["z"]
        later.append(transfer(6 + 2 * side, "y", True, p_ref.at[inner, 8, plane],
                              p_ref.at[inner, 0, plane], has))
        later.append(transfer(7 + 2 * side, "y", False, p_ref.at[inner, 1, plane],
                              p_ref.at[inner, 9, plane], has))
        arrive["x1", side] = (
            transfer(10 + 2 * side, "x", True, p_ref.at[8, inner, plane],
                     p_ref.at[0, inner, plane], has),
            transfer(11 + 2 * side, "x", False, p_ref.at[1, inner, plane],
                     p_ref.at[9, inner, plane], has))
    arrive["y", 0]()
    arrive["y", 1]()
    for done in later:
        done()
    last = []
    for side, plane in ((0, 0), (1, 9)):
        has = low["y"] if side == 0 else high["y"]
        last.append(transfer(14 + 2 * side, "x", True, p_ref.at[8, plane], p_ref.at[0, plane], has))
        last.append(transfer(15 + 2 * side, "x", False, p_ref.at[1, plane], p_ref.at[9, plane], has))
    own.wait()
    arrive["x", 0]()
    arrive["x", 1]()
    for side in (0, 1):
        for done in arrive["x1", side]:
            done()
    for done in last:
        done()
    for sends, copy in pending:
        pl.when(sends)(copy.wait_send)


def padded_volume(volume):
    return pl.pallas_call(
        halo_kernel,
        out_shape=jax.ShapeDtypeStruct((10, 10, 6) + volume.shape[3:], volume.dtype),
        in_specs=[pl.BlockSpec(memory_space=pltpu.VMEM)],
        out_specs=pl.BlockSpec(memory_space=pltpu.VMEM),
        scratch_shapes=[
            pltpu.SemaphoreType.DMA,
            pltpu.SemaphoreType.DMA((18,)),
            pltpu.SemaphoreType.DMA((18,)),
        ],
        compiler_params=pltpu.CompilerParams(collective_id=0, has_side_effects=True),
        name="halo",
    )(volume)


def tiles(array):
    rows, columns = array.shape
    cut = array.reshape(rows // 8, 8, columns // 128, 128).transpose(0, 2, 1, 3)
    return cut.reshape(rows * columns // 128, 128)


def untiled(array, rows, columns):
    cut = array.reshape(rows // 8, columns // 128, 8, 128).transpose(0, 2, 1, 3)
    return cut.reshape(rows, columns)


def from_behind(block, axis, distance):
    devices = range(lax.axis_size(axis))
    route = [(i - distance, i) for i in devices if i - distance in devices]
    return lax.ppermute(block, axis, route)


def shortened(array):
    return jax.tree.map(lambda a: a.astype(jnp.bfloat16) if a.dtype == jnp.float32 else a, array)


def smooth_leaky(values):
    return leak_slope * values + (1.0 - leak_slope) * jax.nn.softplus(values)


def leaky_derivative(values):
    return leak_slope + (1.0 - leak_slope) * jax.nn.sigmoid(values)


def conv_forward(padded, kernel):
    return lax.conv_general_dilated(
        padded,
        kernel,
        (1, 1, 1),
        "VALID",
        dimension_numbers=("DHWCN", "DHWIO", "DHWCN"),
        preferred_element_type=jnp.float32,
    )


def conv_back_input(padded_grad, kernel):
    flipped = kernel[::-1, ::-1, ::-1]
    return lax.conv_general_dilated(
        padded_grad,
        flipped,
        (1, 1, 1),
        "VALID",
        dimension_numbers=("DHWCN", "DHWOI", "DHWCN"),
        preferred_element_type=jnp.float32,
    )


def conv_back_kernel(padded, gradient):
    return lax.conv_general_dilated(
        padded,
        gradient,
        (1, 1, 1),
        "VALID",
        dimension_numbers=("DHWNC", "DHWOI", "DHWNC"),
        preferred_element_type=jnp.float32,
    )


def pooling(values):
    extent_x, extent_y, extent_z, channels, samples = values.shape
    return values.reshape(
        extent_x // 2, 2, extent_y // 2, 2, extent_z // 2, 2, channels, samples
    ).mean(axis=(1, 3, 5))


def spread(values):
    extent_x, extent_y, extent_z, channels, samples = values.shape
    widened = jnp.broadcast_to(
        values[:, None, :, None, :, None],
        (extent_x, 2, extent_y, 2, extent_z, 2, channels, samples),
    )
    return widened.reshape(2 * extent_x, 2 * extent_y, 2 * extent_z, channels, samples)


def fold_faces(inner, from_below, from_above, axis_dim):
    length = inner.shape[axis_dim]
    first = lax.slice_in_dim(inner, 0, 1, axis=axis_dim) + from_below
    middle = lax.slice_in_dim(inner, 1, length - 1, axis=axis_dim)
    last = lax.slice_in_dim(inner, length - 1, length, axis=axis_dim) + from_above
    return jnp.concatenate([first, middle, last], axis=axis_dim)


def body(volume, conv_kernel, dense_one, dense_two, dense_three, targets):
    padded = padded_volume(volume)
    conv_out = conv_forward(padded, conv_kernel)
    pooled = pooling(smooth_leaky(conv_out)).astype(jnp.bfloat16)
    half_x, half_y, half_z, channels, samples = pooled.shape
    groups_y = lax.axis_size("gy")
    groups_z = lax.axis_size("gz")
    groups = groups_y * groups_z
    per_group = channels // groups
    cells = half_x * half_y * half_z
    leaving = pooled.reshape(cells, groups, per_group, samples).transpose(1, 0, 2, 3)
    arrived = exchange(leaving.reshape(groups, cells * per_group, samples), 1)
    arrived = arrived.reshape(groups_y, groups_z, half_x, half_y, half_z, per_group, samples)
    hidden = dense_one.shape[4]
    weights_local = dense_one.reshape(
        half_x, groups_y, half_y, groups_z, half_z, per_group, hidden
    )
    partial_one = jnp.einsum(
        "uvxyzcb,xuyvzch->bh", arrived, weights_local, preferred_element_type=jnp.float32
    )
    pre_one = untiled(all_reduce(tiles(partial_one), 2), samples, hidden)
    hidden_one = smooth_leaky(pre_one)
    pre_two = jnp.dot(hidden_one, dense_two, precision=lax.Precision.HIGHEST)
    hidden_two = smooth_leaky(pre_two)
    prediction = jnp.dot(hidden_two, dense_three, precision=lax.Precision.HIGHEST).T
    error_grad = loss_scale * (prediction - targets)
    grad_pre_two = jnp.dot(
        error_grad.T, dense_three.T, precision=lax.Precision.HIGHEST
    ) * leaky_derivative(pre_two)
    grad_pre_one = (
        jnp.dot(grad_pre_two, dense_two.T, precision=lax.Precision.HIGHEST)
        * leaky_derivative(pre_one)
    ).astype(jnp.bfloat16)
    grad_local = jnp.einsum(
        "uvxyzcb,bh->xuyvzch", arrived, grad_pre_one, preferred_element_type=jnp.float32
    )
    grad_dense_one = (grad_local / samples).astype(jnp.bfloat16).reshape(dense_one.shape)
    grad_arrived = jnp.einsum(
        "xuyvzch,bh->uvxyzcb", weights_local, grad_pre_one, preferred_element_type=jnp.float32
    ).astype(jnp.bfloat16)
    returned = exchange(grad_arrived.reshape(groups, cells * per_group, samples), 3)
    grad_pooled = returned.reshape(groups, cells, per_group, samples).transpose(1, 0, 2, 3)
    grad_pooled = grad_pooled.reshape(half_x, half_y, half_z, channels, samples)
    grad_out = (spread(grad_pooled.astype(jnp.float32)) / 8.0 * leaky_derivative(conv_out)).astype(
        jnp.bfloat16
    )
    widened = jnp.pad(grad_out, ((2, 2), (2, 2), (2, 2), (0, 0), (0, 0)))
    whole = conv_back_input(widened, conv_kernel)
    below_x = from_behind(whole[-1:].astype(jnp.bfloat16), "gx", 1).astype(jnp.float32)
    above_x = from_behind(whole[:1].astype(jnp.bfloat16), "gx", -1).astype(jnp.float32)
    folded = fold_faces(whole[1:-1], below_x, above_x, 0)
    below_y = from_behind(shortened(folded[:, -1:]), "gy", 1)
    above_y = from_behind(shortened(folded[:, :1]), "gy", -1)
    folded = fold_faces(folded[:, 1:-1], below_y, above_y, 1)
    below_z = from_behind(shortened(folded[:, :, -1:]), "gz", 1)
    above_z = from_behind(shortened(folded[:, :, :1]), "gz", -1)
    folded = fold_faces(folded[:, :, 1:-1], below_z, above_z, 2)
    grad_volume = folded.astype(jnp.bfloat16)
    kernel_local = conv_back_kernel(padded, grad_out)
    flat = kernel_local.reshape(-1, 128)
    flat = jnp.concatenate([flat, jnp.zeros((512 - flat.shape[0], 128), flat.dtype)], axis=0)
    grad_conv = all_reduce(flat, 4)[: kernel_local.size // 128].reshape(kernel_local.shape) / samples
    return (prediction, grad_dense_one, grad_conv, grad_volume)


def solution(mesh):
    return jax.shard_map(
        body,
        mesh=mesh,
        in_specs=(
            P("gx", "gy", "gz", None, None),
            P(),
            P("gx", None, None, ("gy", "gz"), None),
            P(),
            P(),
            P(),
        ),
        out_specs=(
            P(),
            P("gx", None, None, ("gy", "gz"), None),
            P(),
            P("gx", "gy", "gz", None, None),
        ),
        check_vma=False,
    )
```

```python
import functools

import jax
import jax.numpy as jnp
from jax import lax
from jax.experimental import pallas as pl
from jax.experimental.pallas import tpu as pltpu
from jax.sharding import PartitionSpec as P

loss_scale = 1024.0
leak_slope = 0.3
MESH = pl.DeviceIdType.MESH


def position():
    gx, gy, gz = lax.axis_index("gx"), lax.axis_index("gy"), lax.axis_index("gz")
    return gx, gy, gz


def chip_coordinates(gx, gy, gz):
    return {"x": gz % 4, "y": gx, "z": (gy // 2) * 2 + gz // 4, "c": gy % 2}


def device_of(at):
    return (at["y"], (at["z"] // 2) * 2 + at["c"], (at["z"] % 2) * 4 + at["x"])


def greet(devices):
    barrier = pltpu.get_barrier_semaphore()
    for device in devices:
        pl.semaphore_signal(barrier, inc=1, device_id=device, device_id_type=MESH)
    pl.semaphore_wait(barrier, len(devices))


def all_reduce_kernel(x_ref, o_ref, from_core, half_sum, from_1, sum_1, from_2, sum_2, from_3,
                      core_send, core_recv, send, recv):
    at = chip_coordinates(*position())
    core = at["c"]
    half = x_ref.shape[0] // 2
    color = half // 2
    n1 = color // 4
    routes = (("x", "y", "z"), ("y", "z", "x"))
    by_rows = n1 >= 32
    n2 = (n1 if by_rows else x_ref.shape[1]) // 4

    def quarter(ref, start, index):
        if by_rows:
            return ref.at[pl.ds(start + index * n2, n2)]
        return ref.at[pl.ds(start, n1), pl.ds(pl.multiple_of(index * n2, n2), n2)]

    def peer(dim, step):
        other = dict(at)
        other[dim] = (at[dim] + step) % 4
        return other

    partner = dict(at)
    partner["c"] = 1 - core
    greet([device_of(partner)] + [device_of(peer(d, s)) for d in "xyz" for s in (1, 2, 3)])

    def copy(src, dst, s_sem, r_sem, device):
        return pltpu.make_async_remote_copy(
            src_ref=src, dst_ref=dst, send_sem=s_sem, recv_sem=r_sem,
            device_id=device, device_id_type=MESH)

    first = copy(x_ref.at[pl.ds((1 - core) * half, half)], from_core, core_send.at[0],
                 core_recv.at[0], device_of(partner))
    first.start()
    first.wait()
    half_sum[...] = x_ref[pl.ds(core * half, half)] + from_core[...]

    def exchange(stage, source, target):
        copies = []
        for k in range(2):
            for s in (2, 1, 3):
                other = peer(routes[k][min(stage, 4 - stage)], s)
                c = copy(source(k, other), target(k, s), send.at[k, stage, s - 1],
                         recv.at[k, stage, s - 1], device_of(other))
                c.start()
                copies.append(c)
        for c in copies:
            c.wait()

    def me(k, j):
        return at[routes[k][j]]

    def first_row(k):
        return pl.multiple_of(k * color + me(k, 0) * n1, n1)

    exchange(0, lambda k, o: half_sum.at[pl.ds(k * color + o[routes[k][0]] * n1, n1)],
             lambda k, s: from_1.at[k, s - 1])
    for k in range(2):
        sum_1[k] = (half_sum[pl.ds(first_row(k), n1)] + from_1[k, 0]
                    + from_1[k, 1] + from_1[k, 2])
    exchange(1, lambda k, o: quarter(sum_1.at[k], 0, o[routes[k][1]]),
             lambda k, s: from_2.at[k, s - 1])
    for k in range(2):
        sum_2[k] = (quarter(sum_1.at[k], 0, me(k, 1))[...] + from_2[k, 0]
                    + from_2[k, 1] + from_2[k, 2])
        from_3[k, me(k, 2)] = sum_2[k]
    exchange(2, lambda k, o: sum_2.at[k], lambda k, s: from_3.at[k, me(k, 2)])
    base = [pl.multiple_of(core * half + first_row(k), n1) for k in range(2)]
    done = [quarter(o_ref, base[k], me(k, 1)) for k in range(2)]
    for k in range(2):
        done[k][...] = from_3[k, 0] + from_3[k, 1] + from_3[k, 2] + from_3[k, 3]
    exchange(3, lambda k, o: done[k], lambda k, s: done[k])
    rows = [o_ref.at[pl.ds(base[k], n1)] for k in range(2)]
    exchange(4, lambda k, o: rows[k], lambda k, s: rows[k])
    mine = o_ref.at[pl.ds(core * half, half)]
    last = copy(mine, mine, core_send.at[1], core_recv.at[1], device_of(partner))
    last.start()
    last.wait()


def all_reduce(x, collective):
    half, lanes = x.shape[0] // 2, x.shape[1]
    n1 = half // 8
    piece = (n1 // 4, lanes) if n1 >= 32 else (n1, lanes // 4)
    f32 = jnp.float32
    return pl.pallas_call(
        all_reduce_kernel,
        out_shape=jax.ShapeDtypeStruct(x.shape, f32),
        in_specs=[pl.BlockSpec(memory_space=pltpu.VMEM)],
        out_specs=pl.BlockSpec(memory_space=pltpu.VMEM),
        scratch_shapes=[
            pltpu.VMEM((half, lanes), f32),
            pltpu.VMEM((half, lanes), f32),
            pltpu.VMEM((2, 3, n1, lanes), f32),
            pltpu.VMEM((2, n1, lanes), f32),
            pltpu.VMEM((2, 3) + piece, f32),
            pltpu.VMEM((2,) + piece, f32),
            pltpu.VMEM((2, 4) + piece, f32),
            pltpu.SemaphoreType.DMA((2,)),
            pltpu.SemaphoreType.DMA((2,)),
            pltpu.SemaphoreType.DMA((2, 5, 3)),
            pltpu.SemaphoreType.DMA((2, 5, 3)),
        ],
        compiler_params=pltpu.CompilerParams(collective_id=collective, has_side_effects=True),
        name="all_reduce_%d" % collective,
    )(x)


def exchange_kernel(pick, place, s_ref, r_ref, own_sem, send, recv):
    gx, gy, gz = position()
    me = gy * 8 + gz

    def device(p):
        return (gx, p // 8, p % 8)

    barrier = pltpu.get_barrier_semaphore()

    def hello(k, carry):
        pl.semaphore_signal(barrier, inc=1, device_id=device((me + k) % 32), device_id_type=MESH)
        return carry

    lax.fori_loop(1, 32, hello, 0)
    own = pltpu.make_async_copy(pick(s_ref, me), place(r_ref, me), own_sem)
    own.start()
    pl.semaphore_wait(barrier, 31)

    def copy(k, source, target, to):
        return pltpu.make_async_remote_copy(
            src_ref=pick(s_ref, source), dst_ref=place(r_ref, target), send_sem=send.at[k],
            recv_sem=recv.at[k], device_id=device(to), device_id_type=MESH)

    def start(k, carry):
        p = (me + ORDER * k) % 32
        copy(k, p, me, p).start()
        return carry

    lax.fori_loop(1, 32, start, 0)

    def finish(k, carry):
        p = (me + ORDER * k) % 32
        q = (me + 32 * ORDER - ORDER * k) % 32
        copy(k, p, q, p).wait_send()
        copy(k, p, q, p).wait_recv()
        return carry

    lax.fori_loop(1, 32, finish, 0)
    own.wait()


ORDER = 11


def by_channels(ref, p):
    return ref.at[:, :, :, p]


def by_cells(ref, p):
    return ref.at[:, p // 8, :, p % 8]


def exchange(blocks, shape, pick, place, collective):
    return pl.pallas_call(
        functools.partial(exchange_kernel, pick, place),
        out_shape=jax.ShapeDtypeStruct(shape, blocks.dtype),
        in_specs=[pl.BlockSpec(memory_space=pltpu.VMEM)],
        out_specs=pl.BlockSpec(memory_space=pltpu.VMEM),
        scratch_shapes=[
            pltpu.SemaphoreType.DMA,
            pltpu.SemaphoreType.DMA((32,)),
            pltpu.SemaphoreType.DMA((32,)),
        ],
        compiler_params=pltpu.CompilerParams(collective_id=collective, has_side_effects=True),
        name="exchange_%d" % collective,
    )(blocks)


def halo_kernel(v_ref, p_ref, own_sem, send, recv):
    gx, gy, gz = position()
    here = {"x": gx, "y": gy, "z": gz}
    size = {"x": 4, "y": 4, "z": 8}
    low = {d: here[d] > 0 for d in "xyz"}
    high = {d: here[d] < size[d] - 1 for d in "xyz"}

    def neighbour(d, step):
        to = dict(here)
        to[d] = (here[d] + size[d] + step) % size[d]
        return (to["x"], to["y"], to["z"])

    zero = jnp.zeros((), p_ref.dtype)

    @pl.when(jnp.logical_not(low["z"]))
    def _():
        p_ref[:, :, 0] = jnp.full(p_ref.shape[:2] + p_ref.shape[3:], zero)

    @pl.when(jnp.logical_not(high["z"]))
    def _():
        p_ref[:, :, 5] = jnp.full(p_ref.shape[:2] + p_ref.shape[3:], zero)

    @pl.when(jnp.logical_not(low["y"]))
    def _():
        p_ref[:, 0] = jnp.full(p_ref.shape[:1] + p_ref.shape[2:], zero)

    @pl.when(jnp.logical_not(high["y"]))
    def _():
        p_ref[:, 9] = jnp.full(p_ref.shape[:1] + p_ref.shape[2:], zero)

    @pl.when(jnp.logical_not(low["x"]))
    def _():
        p_ref[0] = jnp.full(p_ref.shape[1:], zero)

    @pl.when(jnp.logical_not(high["x"]))
    def _():
        p_ref[9] = jnp.full(p_ref.shape[1:], zero)

    greet([neighbour(d, s) for d in "xyz" for s in (1, -1)])
    inner = pl.ds(1, 8)
    mid = pl.ds(1, 4)
    own = pltpu.make_async_copy(v_ref, p_ref.at[inner, inner, mid], own_sem)
    own.start()

    pending = []

    def transfer(slot, d, up, source, target, extra):
        copy = pltpu.make_async_remote_copy(
            src_ref=source, dst_ref=target, send_sem=send.at[slot], recv_sem=recv.at[slot],
            device_id=neighbour(d, 1 if up else -1), device_id_type=MESH)
        sends = high[d] if up else low[d]
        gets = low[d] if up else high[d]
        if extra is not None:
            sends, gets = jnp.logical_and(sends, extra), jnp.logical_and(gets, extra)
        pl.when(sends)(copy.start)
        pending.append((sends, copy))
        return lambda: pl.when(gets)(copy.wait_recv)

    arrive = {}
    arrive["z", 0] = transfer(0, "z", True, v_ref.at[:, :, 3], p_ref.at[inner, inner, 0], None)
    arrive["z", 1] = transfer(1, "z", False, v_ref.at[:, :, 0], p_ref.at[inner, inner, 5], None)
    arrive["y", 0] = transfer(2, "y", True, v_ref.at[:, 7], p_ref.at[inner, 0, mid], None)
    arrive["y", 1] = transfer(3, "y", False, v_ref.at[:, 0], p_ref.at[inner, 9, mid], None)
    arrive["x", 0] = transfer(4, "x", True, v_ref.at[7], p_ref.at[0, inner, mid], None)
    arrive["x", 1] = transfer(5, "x", False, v_ref.at[0], p_ref.at[9, inner, mid], None)

    later = []
    for side, plane in ((0, 0), (1, 5)):
        arrive["z", side]()
        has = low["z"] if side == 0 else high["z"]
        later.append(transfer(6 + 2 * side, "y", True, p_ref.at[inner, 8, plane],
                              p_ref.at[inner, 0, plane], has))
        later.append(transfer(7 + 2 * side, "y", False, p_ref.at[inner, 1, plane],
                              p_ref.at[inner, 9, plane], has))
        arrive["x1", side] = (
            transfer(10 + 2 * side, "x", True, p_ref.at[8, inner, plane],
                     p_ref.at[0, inner, plane], has),
            transfer(11 + 2 * side, "x", False, p_ref.at[1, inner, plane],
                     p_ref.at[9, inner, plane], has))
    arrive["y", 0]()
    arrive["y", 1]()
    for done in later:
        done()
    last = []
    for side, plane in ((0, 0), (1, 9)):
        has = low["y"] if side == 0 else high["y"]
        last.append(transfer(14 + 2 * side, "x", True, p_ref.at[8, plane], p_ref.at[0, plane], has))
        last.append(transfer(15 + 2 * side, "x", False, p_ref.at[1, plane], p_ref.at[9, plane], has))
    own.wait()
    arrive["x", 0]()
    arrive["x", 1]()
    for side in (0, 1):
        for done in arrive["x1", side]:
            done()
    for done in last:
        done()
    for sends, copy in pending:
        pl.when(sends)(copy.wait_send)


def padded_volume(volume):
    return pl.pallas_call(
        halo_kernel,
        out_shape=jax.ShapeDtypeStruct((10, 10, 6) + volume.shape[3:], volume.dtype),
        in_specs=[pl.BlockSpec(memory_space=pltpu.VMEM)],
        out_specs=pl.BlockSpec(memory_space=pltpu.VMEM),
        scratch_shapes=[
            pltpu.SemaphoreType.DMA,
            pltpu.SemaphoreType.DMA((18,)),
            pltpu.SemaphoreType.DMA((18,)),
        ],
        compiler_params=pltpu.CompilerParams(collective_id=0, has_side_effects=True),
        name="halo",
    )(volume)


def dense_forward_kernel(a_ref, w_ref, o_ref):
    rows = a_ref.shape[0]
    block = w_ref[...].reshape(rows, w_ref.shape[2])
    part = lax.dot_general(
        a_ref[...], block, (((0,), (0,)), ((), ())), preferred_element_type=jnp.float32)

    @pl.when(pl.program_id(0) == 0)
    def _():
        o_ref[...] = part

    @pl.when(pl.program_id(0) > 0)
    def _():
        o_ref[...] += part


def dense_forward(features, weights, steps=4):
    rows, samples = features.shape
    hidden = weights.shape[2]
    n = rows // steps
    return pl.pallas_call(
        dense_forward_kernel,
        out_shape=jax.ShapeDtypeStruct((samples, hidden), jnp.float32),
        grid=(steps,),
        in_specs=[pl.BlockSpec((n, samples), lambda i: (i, 0)),
                  pl.BlockSpec((n // 2, 2, hidden), lambda i: (i, 0, 0))],
        out_specs=pl.BlockSpec((samples, hidden), lambda i: (0, 0)),
        name="dense_forward",
    )(features, weights)


def dense_backward_kernel(scale, a_ref, w_ref, g_ref, gt_ref, d_ref, f_ref):
    rows = a_ref.shape[0]
    block = w_ref[...].reshape(rows, w_ref.shape[2])
    f_ref[...] = jnp.dot(block, gt_ref[...], preferred_element_type=jnp.float32).astype(f_ref.dtype)
    part = jnp.dot(a_ref[...], g_ref[...], preferred_element_type=jnp.float32) * scale
    d_ref[...] = part.astype(d_ref.dtype).reshape(d_ref.shape)


def dense_backward(features, weights, grad, steps=4):
    rows, samples = features.shape
    hidden = weights.shape[2]
    n = rows // steps
    return pl.pallas_call(
        functools.partial(dense_backward_kernel, 1.0 / samples),
        out_shape=(jax.ShapeDtypeStruct(weights.shape, jnp.bfloat16),
                   jax.ShapeDtypeStruct(features.shape, jnp.bfloat16)),
        grid=(steps,),
        in_specs=[pl.BlockSpec((n, samples), lambda i: (i, 0)),
                  pl.BlockSpec((n // 2, 2, hidden), lambda i: (i, 0, 0)),
                  pl.BlockSpec((samples, hidden), lambda i: (0, 0)),
                  pl.BlockSpec((hidden, samples), lambda i: (0, 0))],
        out_specs=(pl.BlockSpec((n // 2, 2, hidden), lambda i: (i, 0, 0)),
                   pl.BlockSpec((n, samples), lambda i: (i, 0))),
        name="dense_backward",
    )(features, weights, grad, grad.T)


def from_behind(block, axis, distance):
    devices = range(lax.axis_size(axis))
    route = [(i - distance, i) for i in devices if i - distance in devices]
    return lax.ppermute(block, axis, route)


def shortened(array):
    return jax.tree.map(lambda a: a.astype(jnp.bfloat16) if a.dtype == jnp.float32 else a, array)


def smooth_leaky(values):
    return leak_slope * values + (1.0 - leak_slope) * jax.nn.softplus(values)


def leaky_derivative(values):
    return leak_slope + (1.0 - leak_slope) * jax.nn.sigmoid(values)


def conv_forward(padded, kernel):
    return lax.conv_general_dilated(
        padded,
        kernel,
        (1, 1, 1),
        "VALID",
        dimension_numbers=("DHWCN", "DHWIO", "DHWCN"),
        preferred_element_type=jnp.float32,
    )


def conv_back_input(padded_grad, kernel):
    flipped = kernel[::-1, ::-1, ::-1]
    return lax.conv_general_dilated(
        padded_grad,
        flipped,
        (1, 1, 1),
        "VALID",
        dimension_numbers=("DHWCN", "DHWOI", "DHWCN"),
        preferred_element_type=jnp.float32,
    )


def conv_back_kernel(padded, gradient):
    return lax.conv_general_dilated(
        padded,
        gradient,
        (1, 1, 1),
        "VALID",
        dimension_numbers=("DHWNC", "DHWOI", "DHWNC"),
        preferred_element_type=jnp.float32,
    )


def pooling(values):
    extent_x, extent_y, extent_z, channels, samples = values.shape
    return values.reshape(
        extent_x // 2, 2, extent_y // 2, 2, extent_z // 2, 2, channels, samples
    ).mean(axis=(1, 3, 5))


def spread(values):
    extent_x, extent_y, extent_z, channels, samples = values.shape
    widened = jnp.broadcast_to(
        values[:, None, :, None, :, None],
        (extent_x, 2, extent_y, 2, extent_z, 2, channels, samples),
    )
    return widened.reshape(2 * extent_x, 2 * extent_y, 2 * extent_z, channels, samples)


def fold_faces(inner, from_below, from_above, axis_dim):
    length = inner.shape[axis_dim]
    first = lax.slice_in_dim(inner, 0, 1, axis=axis_dim) + from_below
    middle = lax.slice_in_dim(inner, 1, length - 1, axis=axis_dim)
    last = lax.slice_in_dim(inner, length - 1, length, axis=axis_dim) + from_above
    return jnp.concatenate([first, middle, last], axis=axis_dim)


def body(volume, conv_kernel, dense_one, dense_two, dense_three, targets):
    padded = padded_volume(volume)
    conv_out = conv_forward(padded, conv_kernel)
    pooled = pooling(smooth_leaky(conv_out)).astype(jnp.bfloat16)
    half_x, half_y, half_z, channels, samples = pooled.shape
    groups_y = lax.axis_size("gy")
    groups_z = lax.axis_size("gz")
    groups = groups_y * groups_z
    per_group = channels // groups
    by_group = (half_x, half_y, half_z, groups, per_group, samples)
    by_cell = (half_x, groups_y, half_y, groups_z, half_z, per_group, samples)
    arrived = exchange(pooled.reshape(by_group), by_cell, by_channels, by_cells, 1)
    features = arrived.reshape(-1, samples)
    hidden = dense_one.shape[4]
    weights_local = dense_one.reshape(-1, per_group, hidden)
    pre_one = all_reduce(dense_forward(features, weights_local), 2)
    hidden_one = smooth_leaky(pre_one)
    pre_two = jnp.dot(hidden_one, dense_two, precision=lax.Precision.HIGHEST)
    hidden_two = smooth_leaky(pre_two)
    prediction = jnp.dot(hidden_two, dense_three, precision=lax.Precision.HIGHEST).T
    error_grad = loss_scale * (prediction - targets)
    grad_pre_two = jnp.dot(
        error_grad.T, dense_three.T, precision=lax.Precision.HIGHEST
    ) * leaky_derivative(pre_two)
    grad_pre_one = (
        jnp.dot(grad_pre_two, dense_two.T, precision=lax.Precision.HIGHEST)
        * leaky_derivative(pre_one)
    ).astype(jnp.bfloat16)
    grad_dense_one, grad_features = dense_backward(features, weights_local, grad_pre_one)
    grad_dense_one = grad_dense_one.reshape(dense_one.shape)
    returned = exchange(grad_features.reshape(by_cell), by_group, by_cells, by_channels, 3)
    grad_pooled = returned.reshape(half_x, half_y, half_z, channels, samples)
    grad_out = (spread(grad_pooled.astype(jnp.float32)) / 8.0 * leaky_derivative(conv_out)).astype(
        jnp.bfloat16
    )
    widened = jnp.pad(grad_out, ((2, 2), (2, 2), (2, 2), (0, 0), (0, 0)))
    whole = conv_back_input(widened, conv_kernel)
    below_x = from_behind(whole[-1:].astype(jnp.bfloat16), "gx", 1).astype(jnp.float32)
    above_x = from_behind(whole[:1].astype(jnp.bfloat16), "gx", -1).astype(jnp.float32)
    folded = fold_faces(whole[1:-1], below_x, above_x, 0)
    below_y = from_behind(shortened(folded[:, -1:]), "gy", 1)
    above_y = from_behind(shortened(folded[:, :1]), "gy", -1)
    folded = fold_faces(folded[:, 1:-1], below_y, above_y, 1)
    below_z = from_behind(shortened(folded[:, :, -1:]), "gz", 1)
    above_z = from_behind(shortened(folded[:, :, :1]), "gz", -1)
    folded = fold_faces(folded[:, :, 1:-1], below_z, above_z, 2)
    grad_volume = folded.astype(jnp.bfloat16)
    kernel_local = conv_back_kernel(padded, grad_out)
    flat = kernel_local.reshape(-1, 128)
    flat = jnp.concatenate([flat, jnp.zeros((512 - flat.shape[0], 128), flat.dtype)], axis=0)
    grad_conv = all_reduce(flat, 4)[: kernel_local.size // 128].reshape(kernel_local.shape) / samples
    return (prediction, grad_dense_one, grad_conv, grad_volume)


def solution(mesh):
    return jax.shard_map(
        body,
        mesh=mesh,
        in_specs=(
            P("gx", "gy", "gz", None, None),
            P(),
            P("gx", None, None, ("gy", "gz"), None),
            P(),
            P(),
            P(),
        ),
        out_specs=(
            P(),
            P("gx", None, None, ("gy", "gz"), None),
            P(),
            P("gx", "gy", "gz", None, None),
        ),
        check_vma=False,
    )
```

```python
import functools

import jax
import jax.numpy as jnp
from jax import lax
from jax.experimental import pallas as pl
from jax.experimental.pallas import tpu as pltpu
from jax.sharding import PartitionSpec as P

loss_scale = 1024.0
leak_slope = 0.3
MESH = pl.DeviceIdType.MESH


def position():
    gx, gy, gz = lax.axis_index("gx"), lax.axis_index("gy"), lax.axis_index("gz")
    return gx, gy, gz


def chip_coordinates(gx, gy, gz):
    return {"x": gz % 4, "y": gx, "z": (gy // 2) * 2 + gz // 4, "c": gy % 2}


def device_of(at):
    return (at["y"], (at["z"] // 2) * 2 + at["c"], (at["z"] % 2) * 4 + at["x"])


def greet(devices):
    barrier = pltpu.get_barrier_semaphore()
    for device in devices:
        pl.semaphore_signal(barrier, inc=1, device_id=device, device_id_type=MESH)
    pl.semaphore_wait(barrier, len(devices))


def all_reduce_kernel(x_ref, o_ref, from_core, half_sum, from_1, sum_1, from_2, sum_2, from_3,
                      core_send, core_recv, send, recv):
    at = chip_coordinates(*position())
    core = at["c"]
    half = x_ref.shape[0] // 2
    color = half // 2
    n1 = color // 4
    routes = (("x", "y", "z"), ("y", "z", "x"))
    by_rows = n1 >= 32
    n2 = (n1 if by_rows else x_ref.shape[1]) // 4

    def quarter(ref, start, index):
        if by_rows:
            return ref.at[pl.ds(start + index * n2, n2)]
        return ref.at[pl.ds(start, n1), pl.ds(pl.multiple_of(index * n2, n2), n2)]

    def peer(dim, step):
        other = dict(at)
        other[dim] = (at[dim] + step) % 4
        return other

    partner = dict(at)
    partner["c"] = 1 - core
    greet([device_of(partner)] + [device_of(peer(d, s)) for d in "xyz" for s in (1, 2, 3)])

    def copy(src, dst, s_sem, r_sem, device):
        return pltpu.make_async_remote_copy(
            src_ref=src, dst_ref=dst, send_sem=s_sem, recv_sem=r_sem,
            device_id=device, device_id_type=MESH)

    first = copy(x_ref.at[pl.ds((1 - core) * half, half)], from_core, core_send.at[0],
                 core_recv.at[0], device_of(partner))
    first.start()
    first.wait()
    half_sum[...] = x_ref[pl.ds(core * half, half)] + from_core[...]

    def exchange(stage, source, target):
        copies = []
        for k in range(2):
            for s in (2, 1, 3):
                other = peer(routes[k][min(stage, 4 - stage)], s)
                c = copy(source(k, other), target(k, s), send.at[k, stage, s - 1],
                         recv.at[k, stage, s - 1], device_of(other))
                c.start()
                copies.append(c)
        for c in copies:
            c.wait()

    def me(k, j):
        return at[routes[k][j]]

    def first_row(k):
        return pl.multiple_of(k * color + me(k, 0) * n1, n1)

    exchange(0, lambda k, o: half_sum.at[pl.ds(k * color + o[routes[k][0]] * n1, n1)],
             lambda k, s: from_1.at[k, s - 1])
    for k in range(2):
        sum_1[k] = (half_sum[pl.ds(first_row(k), n1)] + from_1[k, 0]
                    + from_1[k, 1] + from_1[k, 2])
    exchange(1, lambda k, o: quarter(sum_1.at[k], 0, o[routes[k][1]]),
             lambda k, s: from_2.at[k, s - 1])
    for k in range(2):
        sum_2[k] = (quarter(sum_1.at[k], 0, me(k, 1))[...] + from_2[k, 0]
                    + from_2[k, 1] + from_2[k, 2])
        from_3[k, me(k, 2)] = sum_2[k]
    exchange(2, lambda k, o: sum_2.at[k], lambda k, s: from_3.at[k, me(k, 2)])
    base = [pl.multiple_of(core * half + first_row(k), n1) for k in range(2)]
    done = [quarter(o_ref, base[k], me(k, 1)) for k in range(2)]
    for k in range(2):
        done[k][...] = from_3[k, 0] + from_3[k, 1] + from_3[k, 2] + from_3[k, 3]
    exchange(3, lambda k, o: done[k], lambda k, s: done[k])
    rows = [o_ref.at[pl.ds(base[k], n1)] for k in range(2)]
    exchange(4, lambda k, o: rows[k], lambda k, s: rows[k])
    mine = o_ref.at[pl.ds(core * half, half)]
    last = copy(mine, mine, core_send.at[1], core_recv.at[1], device_of(partner))
    last.start()
    last.wait()


def all_reduce(x, collective):
    half, lanes = x.shape[0] // 2, x.shape[1]
    n1 = half // 8
    piece = (n1 // 4, lanes) if n1 >= 32 else (n1, lanes // 4)
    f32 = jnp.float32
    return pl.pallas_call(
        all_reduce_kernel,
        out_shape=jax.ShapeDtypeStruct(x.shape, f32),
        in_specs=[pl.BlockSpec(memory_space=pltpu.VMEM)],
        out_specs=pl.BlockSpec(memory_space=pltpu.VMEM),
        scratch_shapes=[
            pltpu.VMEM((half, lanes), f32),
            pltpu.VMEM((half, lanes), f32),
            pltpu.VMEM((2, 3, n1, lanes), f32),
            pltpu.VMEM((2, n1, lanes), f32),
            pltpu.VMEM((2, 3) + piece, f32),
            pltpu.VMEM((2,) + piece, f32),
            pltpu.VMEM((2, 4) + piece, f32),
            pltpu.SemaphoreType.DMA((2,)),
            pltpu.SemaphoreType.DMA((2,)),
            pltpu.SemaphoreType.DMA((2, 5, 3)),
            pltpu.SemaphoreType.DMA((2, 5, 3)),
        ],
        compiler_params=pltpu.CompilerParams(collective_id=collective, has_side_effects=True),
        name="all_reduce_%d" % collective,
    )(x)


def exchange_kernel(pick, place, s_ref, r_ref, own_sem, send, recv):
    gx, gy, gz = position()
    me = gy * 8 + gz

    def device(p):
        return (gx, p // 8, p % 8)

    barrier = pltpu.get_barrier_semaphore()

    def hello(k, carry):
        pl.semaphore_signal(barrier, inc=1, device_id=device((me + k) % 32), device_id_type=MESH)
        return carry

    lax.fori_loop(1, 32, hello, 0)
    own = pltpu.make_async_copy(pick(s_ref, me), place(r_ref, me), own_sem)
    own.start()
    pl.semaphore_wait(barrier, 31)

    def copy(k, source, target, to):
        return pltpu.make_async_remote_copy(
            src_ref=pick(s_ref, source), dst_ref=place(r_ref, target), send_sem=send.at[k],
            recv_sem=recv.at[k], device_id=device(to), device_id_type=MESH)

    def start(k, carry):
        p = (me + ORDER * k) % 32
        copy(k, p, me, p).start()
        return carry

    lax.fori_loop(1, 32, start, 0)

    def finish(k, carry):
        p = (me + ORDER * k) % 32
        q = (me + 32 * ORDER - ORDER * k) % 32
        copy(k, p, q, p).wait_send()
        copy(k, p, q, p).wait_recv()
        return carry

    lax.fori_loop(1, 32, finish, 0)
    own.wait()


ORDER = 11


def by_channels(ref, p):
    return ref.at[:, :, :, p]


def by_cells(ref, p):
    return ref.at[:, p // 8, :, p % 8]


def exchange(blocks, shape, pick, place, collective):
    return pl.pallas_call(
        functools.partial(exchange_kernel, pick, place),
        out_shape=jax.ShapeDtypeStruct(shape, blocks.dtype),
        in_specs=[pl.BlockSpec(memory_space=pltpu.VMEM)],
        out_specs=pl.BlockSpec(memory_space=pltpu.VMEM),
        scratch_shapes=[
            pltpu.SemaphoreType.DMA,
            pltpu.SemaphoreType.DMA((32,)),
            pltpu.SemaphoreType.DMA((32,)),
        ],
        compiler_params=pltpu.CompilerParams(collective_id=collective, has_side_effects=True),
        name="exchange_%d" % collective,
    )(blocks)


def halo_kernel(v_ref, p_ref, own_sem, send, recv):
    gx, gy, gz = position()
    here = {"x": gx, "y": gy, "z": gz}
    size = {"x": 4, "y": 4, "z": 8}
    low = {d: here[d] > 0 for d in "xyz"}
    high = {d: here[d] < size[d] - 1 for d in "xyz"}

    def neighbour(d, step):
        to = dict(here)
        to[d] = (here[d] + size[d] + step) % size[d]
        return (to["x"], to["y"], to["z"])

    zero = jnp.zeros((), p_ref.dtype)

    @pl.when(jnp.logical_not(low["z"]))
    def _():
        p_ref[:, :, 0] = jnp.full(p_ref.shape[:2] + p_ref.shape[3:], zero)

    @pl.when(jnp.logical_not(high["z"]))
    def _():
        p_ref[:, :, 5] = jnp.full(p_ref.shape[:2] + p_ref.shape[3:], zero)

    @pl.when(jnp.logical_not(low["y"]))
    def _():
        p_ref[:, 0] = jnp.full(p_ref.shape[:1] + p_ref.shape[2:], zero)

    @pl.when(jnp.logical_not(high["y"]))
    def _():
        p_ref[:, 9] = jnp.full(p_ref.shape[:1] + p_ref.shape[2:], zero)

    @pl.when(jnp.logical_not(low["x"]))
    def _():
        p_ref[0] = jnp.full(p_ref.shape[1:], zero)

    @pl.when(jnp.logical_not(high["x"]))
    def _():
        p_ref[9] = jnp.full(p_ref.shape[1:], zero)

    greet([neighbour(d, s) for d in "xyz" for s in (1, -1)])
    inner = pl.ds(1, 8)
    mid = pl.ds(1, 4)
    own = pltpu.make_async_copy(v_ref, p_ref.at[inner, inner, mid], own_sem)
    own.start()

    pending = []

    def transfer(slot, d, up, source, target, extra):
        copy = pltpu.make_async_remote_copy(
            src_ref=source, dst_ref=target, send_sem=send.at[slot], recv_sem=recv.at[slot],
            device_id=neighbour(d, 1 if up else -1), device_id_type=MESH)
        sends = high[d] if up else low[d]
        gets = low[d] if up else high[d]
        if extra is not None:
            sends, gets = jnp.logical_and(sends, extra), jnp.logical_and(gets, extra)
        pl.when(sends)(copy.start)
        pending.append((sends, copy))
        return lambda: pl.when(gets)(copy.wait_recv)

    arrive = {}
    arrive["z", 0] = transfer(0, "z", True, v_ref.at[:, :, 3], p_ref.at[inner, inner, 0], None)
    arrive["z", 1] = transfer(1, "z", False, v_ref.at[:, :, 0], p_ref.at[inner, inner, 5], None)
    arrive["y", 0] = transfer(2, "y", True, v_ref.at[:, 7], p_ref.at[inner, 0, mid], None)
    arrive["y", 1] = transfer(3, "y", False, v_ref.at[:, 0], p_ref.at[inner, 9, mid], None)
    arrive["x", 0] = transfer(4, "x", True, v_ref.at[7], p_ref.at[0, inner, mid], None)
    arrive["x", 1] = transfer(5, "x", False, v_ref.at[0], p_ref.at[9, inner, mid], None)

    later = []
    for side, plane in ((0, 0), (1, 5)):
        arrive["z", side]()
        has = low["z"] if side == 0 else high["z"]
        later.append(transfer(6 + 2 * side, "y", True, p_ref.at[inner, 8, plane],
                              p_ref.at[inner, 0, plane], has))
        later.append(transfer(7 + 2 * side, "y", False, p_ref.at[inner, 1, plane],
                              p_ref.at[inner, 9, plane], has))
        arrive["x1", side] = (
            transfer(10 + 2 * side, "x", True, p_ref.at[8, inner, plane],
                     p_ref.at[0, inner, plane], has),
            transfer(11 + 2 * side, "x", False, p_ref.at[1, inner, plane],
                     p_ref.at[9, inner, plane], has))
    arrive["y", 0]()
    arrive["y", 1]()
    for done in later:
        done()
    last = []
    for side, plane in ((0, 0), (1, 9)):
        has = low["y"] if side == 0 else high["y"]
        last.append(transfer(14 + 2 * side, "x", True, p_ref.at[8, plane], p_ref.at[0, plane], has))
        last.append(transfer(15 + 2 * side, "x", False, p_ref.at[1, plane], p_ref.at[9, plane], has))
    own.wait()
    arrive["x", 0]()
    arrive["x", 1]()
    for side in (0, 1):
        for done in arrive["x1", side]:
            done()
    for done in last:
        done()
    for sends, copy in pending:
        pl.when(sends)(copy.wait_send)


def padded_volume(volume):
    return pl.pallas_call(
        halo_kernel,
        out_shape=jax.ShapeDtypeStruct((10, 10, 6) + volume.shape[3:], volume.dtype),
        in_specs=[pl.BlockSpec(memory_space=pltpu.VMEM)],
        out_specs=pl.BlockSpec(memory_space=pltpu.VMEM),
        scratch_shapes=[
            pltpu.SemaphoreType.DMA,
            pltpu.SemaphoreType.DMA((18,)),
            pltpu.SemaphoreType.DMA((18,)),
        ],
        compiler_params=pltpu.CompilerParams(collective_id=0, has_side_effects=True),
        name="halo",
    )(volume)


def dense_forward_kernel(a_ref, w_ref, o_ref):
    rows = a_ref.shape[0]
    block = w_ref[...].reshape(rows, w_ref.shape[2])
    part = lax.dot_general(
        a_ref[...], block, (((0,), (0,)), ((), ())), preferred_element_type=jnp.float32)

    @pl.when(pl.program_id(0) == 0)
    def _():
        o_ref[...] = part

    @pl.when(pl.program_id(0) > 0)
    def _():
        o_ref[...] += part


def dense_forward(features, weights, steps=4):
    rows, samples = features.shape
    hidden = weights.shape[2]
    n = rows // steps
    return pl.pallas_call(
        dense_forward_kernel,
        out_shape=jax.ShapeDtypeStruct((samples, hidden), jnp.float32),
        grid=(steps,),
        in_specs=[pl.BlockSpec((n, samples), lambda i: (i, 0)),
                  pl.BlockSpec((n // 2, 2, hidden), lambda i: (i, 0, 0))],
        out_specs=pl.BlockSpec((samples, hidden), lambda i: (0, 0)),
        name="dense_forward",
    )(features, weights)


def dense_backward_kernel(scale, a_ref, w_ref, g_ref, gt_ref, d_ref, f_ref):
    rows = a_ref.shape[0]
    block = w_ref[...].reshape(rows, w_ref.shape[2])
    f_ref[...] = jnp.dot(block, gt_ref[...], preferred_element_type=jnp.float32).astype(f_ref.dtype)
    part = jnp.dot(a_ref[...], g_ref[...], preferred_element_type=jnp.float32) * scale
    d_ref[...] = part.astype(d_ref.dtype).reshape(d_ref.shape)


def dense_backward(features, weights, grad, steps=4):
    rows, samples = features.shape
    hidden = weights.shape[2]
    n = rows // steps
    return pl.pallas_call(
        functools.partial(dense_backward_kernel, 1.0 / samples),
        out_shape=(jax.ShapeDtypeStruct(weights.shape, jnp.bfloat16),
                   jax.ShapeDtypeStruct(features.shape, jnp.bfloat16)),
        grid=(steps,),
        in_specs=[pl.BlockSpec((n, samples), lambda i: (i, 0)),
                  pl.BlockSpec((n // 2, 2, hidden), lambda i: (i, 0, 0)),
                  pl.BlockSpec((samples, hidden), lambda i: (0, 0)),
                  pl.BlockSpec((hidden, samples), lambda i: (0, 0))],
        out_specs=(pl.BlockSpec((n // 2, 2, hidden), lambda i: (i, 0, 0)),
                   pl.BlockSpec((n, samples), lambda i: (i, 0))),
        name="dense_backward",
    )(features, weights, grad, grad.T)


def fill_band(k_ref, t_ref):
    taps, out = 96, k_ref.shape[1]
    wide = 2 * taps
    for z in range(4):
        row = lax.broadcasted_iota(jnp.int32, (wide, 2 * wide), 0)
        column = lax.broadcasted_iota(jnp.int32, (wide, 2 * wide), 1)
        second = (row >= taps).astype(jnp.int32)
        hit = column == row + 32 * z + second * (wide - taps)
        pick = jnp.where(hit, 1.0, 0.0).astype(k_ref.dtype)
        for t in range(0, 9, 2):
            n = min(2, 9 - t)
            part = lax.dot_general(
                k_ref[t * taps:(t + n) * taps], pick[:n * taps, :n * wide],
                (((0,), (0,)), ((), ())), preferred_element_type=jnp.float32)
            t_ref[z * out:(z + 1) * out, t * wide:(t + n) * wide] = part.astype(t_ref.dtype)


def conv_forward_kernel(k_ref, p_ref, pooled_ref, slope_ref, t_ref):
    fill_band(k_ref, t_ref)
    cells, channels, samples = p_ref.shape[2:]
    rows = cells * channels

    def column(x, y):
        return p_ref[x, y].reshape(rows, samples)

    def block(i, carry):
        bx, by = i // 4, i % 4
        total = None
        for dx in range(2):
            columns = {}
            for ox in range(3):
                for y in range(4):
                    columns[ox, y] = column(2 * bx + dx + ox, 2 * by + y)
            pair = jnp.concatenate(
                [jnp.concatenate([columns[ox, oy], columns[ox, oy + 1]], axis=1)
                 for ox in range(3) for oy in range(3)], axis=0)
            out = jnp.dot(t_ref[...], pair, preferred_element_type=jnp.float32)
            e = jnp.exp(-jnp.abs(out))
            s = 1.0 + e
            act = leak_slope * out + (1.0 - leak_slope) * (jnp.maximum(out, 0.0) + jnp.log(s))
            slope = leak_slope + (1.0 - leak_slope) * (jnp.where(out >= 0.0, 1.0, e) / s)
            slope = slope.astype(slope_ref.dtype)
            for dy in range(2):
                part = slope[:, dy * samples:(dy + 1) * samples]
                slope_ref[2 * bx + dx, 2 * by + dy] = part.reshape(slope_ref.shape[2:])
            total = act if total is None else total + act
        total = total[:, :samples] + total[:, samples:]
        total = total.reshape(2, 2, slope_ref.shape[3], samples)
        pooled_ref[bx, by] = ((total[:, 0] + total[:, 1]) * 0.125).astype(pooled_ref.dtype)
        return carry

    lax.fori_loop(0, 16, block, 0)


def conv_pool(padded, kernel):
    nx, ny, nz, _, samples = padded.shape
    channels = kernel.shape[-1]
    shape = (nx - 2, ny - 2, nz - 2, channels, samples)
    pooled = (shape[0] // 2, shape[1] // 2, shape[2] // 2, channels, samples)
    vmem = pl.BlockSpec(memory_space=pltpu.VMEM)
    return pl.pallas_call(
        conv_forward_kernel,
        out_shape=(jax.ShapeDtypeStruct(pooled, jnp.bfloat16),
                   jax.ShapeDtypeStruct(shape, jnp.bfloat16)),
        in_specs=[vmem, vmem],
        out_specs=(vmem, vmem),
        scratch_shapes=[pltpu.VMEM(((nz - 2) * channels, 9 * nz * padded.shape[3]), jnp.bfloat16)],
        compiler_params=pltpu.CompilerParams(vmem_limit_bytes=48 * 2**20),
        name="conv_pool",
    )(kernel.reshape(-1, channels), padded)


def from_behind(block, axis, distance):
    devices = range(lax.axis_size(axis))
    route = [(i - distance, i) for i in devices if i - distance in devices]
    return lax.ppermute(block, axis, route)


def shortened(array):
    return jax.tree.map(lambda a: a.astype(jnp.bfloat16) if a.dtype == jnp.float32 else a, array)


def smooth_leaky(values):
    return leak_slope * values + (1.0 - leak_slope) * jax.nn.softplus(values)


def leaky_derivative(values):
    return leak_slope + (1.0 - leak_slope) * jax.nn.sigmoid(values)


def conv_back_input(padded_grad, kernel):
    flipped = kernel[::-1, ::-1, ::-1]
    return lax.conv_general_dilated(
        padded_grad,
        flipped,
        (1, 1, 1),
        "VALID",
        dimension_numbers=("DHWCN", "DHWOI", "DHWCN"),
        preferred_element_type=jnp.float32,
    )


def conv_back_kernel(padded, gradient):
    return lax.conv_general_dilated(
        padded,
        gradient,
        (1, 1, 1),
        "VALID",
        dimension_numbers=("DHWNC", "DHWOI", "DHWNC"),
        preferred_element_type=jnp.float32,
    )


def spread(values):
    extent_x, extent_y, extent_z, channels, samples = values.shape
    widened = jnp.broadcast_to(
        values[:, None, :, None, :, None],
        (extent_x, 2, extent_y, 2, extent_z, 2, channels, samples),
    )
    return widened.reshape(2 * extent_x, 2 * extent_y, 2 * extent_z, channels, samples)


def fold_faces(inner, from_below, from_above, axis_dim):
    length = inner.shape[axis_dim]
    first = lax.slice_in_dim(inner, 0, 1, axis=axis_dim) + from_below
    middle = lax.slice_in_dim(inner, 1, length - 1, axis=axis_dim)
    last = lax.slice_in_dim(inner, length - 1, length, axis=axis_dim) + from_above
    return jnp.concatenate([first, middle, last], axis=axis_dim)


def body(volume, conv_kernel, dense_one, dense_two, dense_three, targets):
    padded = padded_volume(volume)
    pooled, slope = conv_pool(padded, conv_kernel)
    half_x, half_y, half_z, channels, samples = pooled.shape
    groups_y = lax.axis_size("gy")
    groups_z = lax.axis_size("gz")
    groups = groups_y * groups_z
    per_group = channels // groups
    by_group = (half_x, half_y, half_z, groups, per_group, samples)
    by_cell = (half_x, groups_y, half_y, groups_z, half_z, per_group, samples)
    arrived = exchange(pooled.reshape(by_group), by_cell, by_channels, by_cells, 1)
    features = arrived.reshape(-1, samples)
    hidden = dense_one.shape[4]
    weights_local = dense_one.reshape(-1, per_group, hidden)
    pre_one = all_reduce(dense_forward(features, weights_local), 2)
    hidden_one = smooth_leaky(pre_one)
    pre_two = jnp.dot(hidden_one, dense_two, precision=lax.Precision.HIGHEST)
    hidden_two = smooth_leaky(pre_two)
    prediction = jnp.dot(hidden_two, dense_three, precision=lax.Precision.HIGHEST).T
    error_grad = loss_scale * (prediction - targets)
    grad_pre_two = jnp.dot(
        error_grad.T, dense_three.T, precision=lax.Precision.HIGHEST
    ) * leaky_derivative(pre_two)
    grad_pre_one = (
        jnp.dot(grad_pre_two, dense_two.T, precision=lax.Precision.HIGHEST)
        * leaky_derivative(pre_one)
    ).astype(jnp.bfloat16)
    grad_dense_one, grad_features = dense_backward(features, weights_local, grad_pre_one)
    grad_dense_one = grad_dense_one.reshape(dense_one.shape)
    returned = exchange(grad_features.reshape(by_cell), by_group, by_cells, by_channels, 3)
    grad_pooled = returned.reshape(half_x, half_y, half_z, channels, samples)
    grad_out = (spread(grad_pooled.astype(jnp.float32)) / 8.0 * slope.astype(jnp.float32)).astype(
        jnp.bfloat16
    )
    widened = jnp.pad(grad_out, ((2, 2), (2, 2), (2, 2), (0, 0), (0, 0)))
    whole = conv_back_input(widened, conv_kernel)
    below_x = from_behind(whole[-1:].astype(jnp.bfloat16), "gx", 1).astype(jnp.float32)
    above_x = from_behind(whole[:1].astype(jnp.bfloat16), "gx", -1).astype(jnp.float32)
    folded = fold_faces(whole[1:-1], below_x, above_x, 0)
    below_y = from_behind(shortened(folded[:, -1:]), "gy", 1)
    above_y = from_behind(shortened(folded[:, :1]), "gy", -1)
    folded = fold_faces(folded[:, 1:-1], below_y, above_y, 1)
    below_z = from_behind(shortened(folded[:, :, -1:]), "gz", 1)
    above_z = from_behind(shortened(folded[:, :, :1]), "gz", -1)
    folded = fold_faces(folded[:, :, 1:-1], below_z, above_z, 2)
    grad_volume = folded.astype(jnp.bfloat16)
    kernel_local = conv_back_kernel(padded, grad_out)
    flat = kernel_local.reshape(-1, 128)
    flat = jnp.concatenate([flat, jnp.zeros((512 - flat.shape[0], 128), flat.dtype)], axis=0)
    grad_conv = all_reduce(flat, 4)[: kernel_local.size // 128].reshape(kernel_local.shape) / samples
    return (prediction, grad_dense_one, grad_conv, grad_volume)


def solution(mesh):
    return jax.shard_map(
        body,
        mesh=mesh,
        in_specs=(
            P("gx", "gy", "gz", None, None),
            P(),
            P("gx", None, None, ("gy", "gz"), None),
            P(),
            P(),
            P(),
        ),
        out_specs=(
            P(),
            P("gx", None, None, ("gy", "gz"), None),
            P(),
            P("gx", "gy", "gz", None, None),
        ),
        check_vma=False,
    )
```
